256 devices in a mesh: coarse: 4 (over y), fine: 8 (over z), group: 8 (over x, core).
Axes of the slice: x: 4, y: 4, z: 8, core: 2. Of those that a mesh axis runs over, the one named last changes fastest.
Arguments:
- fresh_keys: bfloat16 [32, 16384, 8, 128], P(None, ('coarse', 'fine'), 'group'), may hold values from -6 to 6
- fresh_values: bfloat16 [32, 16384, 8, 128], P(None, ('coarse', 'fine'), 'group'), may hold values from -6 to 6
- turn_angle: float32 [16384, 64], replicated, may hold values from -3.140625 to 3.140625
- key_gain: float32 [128], replicated, may hold values from 0.25 to 1.75
Outputs:
- decode_keys: bfloat16 [32, 8, 128, 16384], P(('coarse', 'fine'), 'group')
- decode_values: bfloat16 [32, 16384, 8, 128], P(('coarse', 'fine'), None, 'group')
- key_scale: float32 [32, 8, 128], P(('coarse', 'fine'), 'group')
The draws below stay inside these ranges and needn't reach their ends.
All inputs are finite; a program needn't handle non-finite values. Where the reference program divides by a largest or mean magnitude, that divisor is 1e-20 or more.
Results may differ from the reference program's by a relative error of at most 0.001.
Values may be sent and summed in bfloat16 or wider, within the bound.
A program may use at most 128 MiB of HBM per device.

```python
import jax
import jax.numpy as jnp
from jax import lax

BATCH = 32
LENGTH = 16384
KV_HEADS = 8
HEAD_SIZE = 128
HALF_HEAD = 64


def steps_of(key, dims, pieces, least, largest):
    loudness, own = 1.0, jax.random.fold_in(key, 6)
    for dim, shards_of in pieces:
        draws = jnp.exp(jax.random.uniform(jax.random.fold_in(own, dim), (shards_of,), jnp.float32, least / len(pieces), largest / len(pieces)))
        loudness = loudness * jnp.repeat(draws, dims[dim] // shards_of).reshape([-1 if axis == dim else 1 for axis in range(len(dims))])
    return loudness


def noise(stream_key, extent, scale, limit, shards=(), held_as=jnp.bfloat16):
    factor_of = steps_of(stream_key, extent, shards, -0.22, 0.18) if shards else 1.0
    values = jax.random.normal(stream_key, extent, jnp.float32) * scale * factor_of
    return jnp.minimum(jnp.maximum(values, -limit), limit).astype(held_as)


def setup_inputs(seed: int = 0) -> dict:
    streams_of = jax.random.split(jax.random.key(seed), 5)
    return {
        "fresh_keys": noise(streams_of[0], (BATCH, LENGTH, KV_HEADS, HEAD_SIZE), 1.0, 6.0, ((1, 32), (2, 8))),
        "fresh_values": noise(streams_of[1], (BATCH, LENGTH, KV_HEADS, HEAD_SIZE), 1.0, 6.0, ((1, 32), (2, 8))),
        "turn_angle": jnp.clip(jax.random.uniform(streams_of[2], (LENGTH, HALF_HEAD), jnp.float32, -3.140625, 3.140625), -3.140625, 3.140625),
        "key_gain": jnp.clip(1.0 + 0.15 * jax.random.normal(streams_of[3], (HEAD_SIZE,), jnp.float32), 0.25, 1.75),
    }


def turn_pairs(vectors, angle):
    half = vectors.shape[-1] // 2
    cosine, sine = (jnp.cos(angle)[None, :, None, :], jnp.sin(angle)[None, :, None, :])
    first, second = (vectors[..., :half], vectors[..., half:])
    return jnp.concatenate([first * cosine - second * sine, second * cosine + first * sine], axis=-1)

def root_norm(vectors, row_gain):
    return vectors * lax.rsqrt(lax.optimization_barrier(jnp.mean(vectors * vectors, axis=-1, keepdims=True)) + 1e-06) * row_gain

def ready_to_store(plain_keys, angle, key_gain):
    wide_keys = plain_keys.astype(jnp.float32)
    wide_keys = root_norm(wide_keys, key_gain)
    return turn_pairs(wide_keys, angle)

def reference(fresh_keys, fresh_values, turn_angle, key_gain):
    turned_keys = ready_to_store(fresh_keys, turn_angle, key_gain)
    key_scale = lax.optimization_barrier(jnp.max(jnp.abs(turned_keys), axis=1))
    narrow_keys = (turned_keys / key_scale[:, None]).astype(jnp.bfloat16)
    decode_keys = jnp.transpose(narrow_keys, (0, 2, 3, 1))
    decode_values = fresh_values
    return (decode_keys, decode_values, key_scale)
```

```python
import jax
import jax.numpy as jnp
from jax import lax
from jax.experimental import pallas as pl
from jax.experimental.pallas import tpu as pltpu
from jax.sharding import PartitionSpec as P

MESH = pl.DeviceIdType.MESH
COARSE, FINE = 4, 8
PARTS = COARSE * FINE
CHUNK = 128
KEYS, VALUES = 0, 1
LAG = 3
AHEAD = 4
OFFSETS = (4, 3, -3, 2, -2, 1, -1, 0)
FORWARD4 = ((0, 2), (1, 3))


def coarse_plan():
    plan = []
    for array in (KEYS, VALUES):
        plan += [[(array, 1, o), (array, 3, o)] for o in OFFSETS]
        plan += [[(array, 2, o)] for o in OFFSETS]
    return plan


def fine_plan(way):
    ready = {e: j + LAG + (e[1] == 2) for j, step in enumerate(coarse_plan()) for e in step}
    waiting = []
    for array in (KEYS, VALUES):
        for rows in range(COARSE):
            for hops in range(1, FINE // 2 + 1):
                if hops == FINE // 2 and (rows in FORWARD4[array]) != (way == 1):
                    continue
                off = hops if hops == FINE // 2 else way * hops
                waiting.append((ready.get((array, rows, off), 0), array, hops, rows, 0))
    plan = []
    while waiting:
        now = len(plan)
        best = min(
            (w for w in waiting if w[0] <= now), key=lambda w: (w[1], w[4] - w[2], w[0], w[3])
        )
        waiting.remove(best)
        plan.append(best[1:])
        _, array, hops, rows, done = best
        if done + 1 < hops:
            waiting.append((now + LAG, array, hops, rows, done + 1))
    return plan


COARSE_PLAN = coarse_plan()
FINE_PLAN = {way: fine_plan(way) for way in (1, -1)}
STEPS = len(FINE_PLAN[1])
SLOT = {}
for _step in COARSE_PLAN:
    for _array, _rows, _off in _step:
        if _off:
            SLOT["staged", _array, _rows, _off] = len(SLOT)
for _way in FINE_PLAN:
    for _array, _hops, _rows, _done in FINE_PLAN[_way]:
        if _done:
            SLOT["passing", _way, _array, _hops, _rows, _done] = len(SLOT)
SLOTS = len(SLOT)
FIRST_TURN = STEPS // 2 + LAG + 1
TURNS = 2
FIRST_NARROW = FIRST_TURN + PARTS // TURNS
NARROWS = 4


def kernel(keys, values, angle, gain, out_keys, out_values, out_scale,
           held, turned, angles, peak, gains, box,
           sent, box_came, key_came, value_came, local_sem):
    c, f, g = (lax.axis_index(name) for name in ("coarse", "fine", "group"))
    block = held.shape[1]
    me = c * FINE + f
    source_of = (keys, values)
    final_of = (held, out_values)

    def at(row, column):
        return ((c + row) % COARSE, (f + column + FINE) % FINE, g)

    near = [(0, 1), (0, -1), (1, 0), (3, 0), (2, 0)]
    barrier = pltpu.get_barrier_semaphore()
    for row, column in near:
        pl.semaphore_signal(barrier, inc=1, device_id=at(row, column), device_id_type=MESH)
    pl.semaphore_wait(barrier, len(near))

    def came(array, device):
        return key_came.at[device] if array == KEYS else value_came

    def send_coarse(array, rows, off):
        there = at(rows, 0)
        if off:
            slot = SLOT["staged", array, rows, off]
            target, arrived = box.at[slot], box_came.at[slot]
        else:
            target, arrived = final_of[array].at[me], came(array, me)
        pltpu.make_async_remote_copy(
            src_ref=source_of[array].at[there[0] * FINE + (f + off + FINE) % FINE],
            dst_ref=target, send_sem=sent, recv_sem=arrived, device_id=there, device_id_type=MESH,
        ).start()

    def send_fine(way, array, hops, rows, done):
        off = hops if hops == FINE // 2 else way * hops
        if done:
            slot = SLOT["passing", way, array, hops, rows, done]
        elif rows:
            slot = SLOT["staged", array, rows, off]
        else:
            slot = None
        if slot is None:
            source = source_of[array].at[c * FINE + (f + off + FINE) % FINE]
        else:
            source = box.at[slot]
            pltpu.make_async_copy(source, source, box_came.at[slot]).wait()
        if done + 1 < hops:
            slot = SLOT["passing", way, array, hops, rows, done + 1]
            target, arrived = box.at[slot], box_came.at[slot]
        else:
            home = ((c + COARSE - rows) % COARSE) * FINE + (f - way * done + FINE) % FINE
            target, arrived = final_of[array].at[home], came(array, home)
        pltpu.make_async_remote_copy(
            src_ref=source, dst_ref=target, send_sem=sent, recv_sem=arrived,
            device_id=at(0, way), device_id_type=MESH,
        ).start()

    def exchange(step):
        if step + AHEAD < len(COARSE_PLAN):
            for entry in COARSE_PLAN[step + AHEAD]:
                send_coarse(*entry)
        for way in FINE_PLAN:
            send_fine(way, *FINE_PLAN[way][step])

    def turn(source):
        @pl.loop(0, block // CHUNK)
        def _(n):
            plain = held[source, pl.ds(pl.multiple_of(n * CHUNK, CHUNK), CHUNK), :]
            wide = plain.astype(jnp.float32).T
            mean = jnp.sum(wide * wide, axis=0, keepdims=True) * (1.0 / wide.shape[0])
            wide = wide * lax.rsqrt(mean + 1e-06) * gains[...]
            where = pl.ds(pl.multiple_of(source * block + n * CHUNK, CHUNK), CHUNK)
            a = angles[:, where]
            cosine, sine = jnp.cos(a), jnp.sin(a)
            half = a.shape[0]
            first, second = wide[:half], wide[half:]
            low = first * cosine - second * sine
            high = second * cosine + first * sine
            turned[:half, where] = low
            turned[half:, where] = high
            peak[:half] = jnp.maximum(peak[:half], jnp.abs(low))
            peak[half:] = jnp.maximum(peak[half:], jnp.abs(high))

    def narrow(i):
        where = pl.ds(pl.multiple_of(i * block, block), block)
        scale = jnp.max(peak[...], axis=1, keepdims=True)
        out_keys[:, where] = (turned[:, where] / scale).astype(out_keys.dtype)

    for entry in sum(COARSE_PLAN[:AHEAD], []):
        send_coarse(*entry)
    own_keys = pltpu.make_async_copy(keys.at[me], held.at[me], local_sem.at[0])
    own_values = pltpu.make_async_copy(values.at[me], out_values.at[me], local_sem.at[1])
    get_angles = pltpu.make_async_copy(angle, angles, local_sem.at[2])
    for step in range(FIRST_TURN):
        exchange(step)
        if step == 2:
            own_keys.start()
            own_values.start()
            get_angles.start()
    peak[...] = jnp.zeros_like(peak)
    gains[...] = jnp.broadcast_to(gain[...], gains.shape).T
    own_keys.wait()
    own_values.wait()
    get_angles.wait()
    for i in range(1, PARTS):
        source = (me + i) % PARTS
        pltpu.make_async_copy(held.at[source], held.at[source], key_came.at[source]).wait()

    @pl.loop(FIRST_TURN, STEPS)
    def _(step):
        for k in range(FIRST_TURN, STEPS):
            @pl.when(step == k)
            def _():
                exchange(k)

        @pl.when(step < FIRST_NARROW)
        def _():
            @pl.loop(0, TURNS)
            def _(i):
                turn((step - FIRST_TURN) * TURNS + i)

        @pl.when((step >= FIRST_NARROW) & (step < FIRST_NARROW + PARTS // NARROWS))
        def _():
            @pl.loop(0, NARROWS)
            def _(i):
                narrow((step - FIRST_NARROW) * NARROWS + i)

    out_scale[...] = jnp.max(peak[...].T, axis=0, keepdims=True)
    whole = pl.ds(0, PARTS)
    sends = sum(len(s) for s in COARSE_PLAN) + 2 * STEPS
    for _ in range(sends // PARTS):
        pltpu.make_async_copy(values.at[whole], values.at[whole], sent).wait()
    if sends % PARTS:
        rest = pl.ds(0, sends % PARTS)
        pltpu.make_async_copy(values.at[rest], values.at[rest], sent).wait()
    rest = pl.ds(0, PARTS - 1)
    pltpu.make_async_copy(values.at[rest], values.at[rest], value_came).wait()


def local(fresh_keys, fresh_values, turn_angle, key_gain):
    batch, block, _, size = fresh_keys.shape
    length = turn_angle.shape[0]
    hbm = pl.BlockSpec(memory_space=pltpu.HBM)
    vmem = pl.BlockSpec(memory_space=pltpu.VMEM)
    out_keys, out_values, out_scale = pl.pallas_call(
        kernel,
        name="exchange",
        out_shape=[
            pltpu.VMEM((size, length), jnp.bfloat16),
            pltpu.VMEM((batch, block, size), jnp.bfloat16),
            jax.ShapeDtypeStruct((1, size), jnp.float32),
        ],
        in_specs=[hbm, hbm, hbm, vmem],
        out_specs=[vmem, vmem, vmem],
        scratch_shapes=[
            pltpu.VMEM((batch, block, size), jnp.bfloat16),
            pltpu.VMEM((size, length), jnp.float32),
            pltpu.VMEM((size // 2, length), jnp.float32),
            pltpu.VMEM((size, CHUNK), jnp.float32),
            pltpu.VMEM((size, CHUNK), jnp.float32),
            pltpu.VMEM((SLOTS, block, size), jnp.bfloat16),
            pltpu.SemaphoreType.DMA,
            pltpu.SemaphoreType.DMA((SLOTS,)),
            pltpu.SemaphoreType.DMA((PARTS,)),
            pltpu.SemaphoreType.DMA,
            pltpu.SemaphoreType.DMA((3,)),
        ],
        compiler_params=pltpu.CompilerParams(
            collective_id=0, has_side_effects=True, vmem_limit_bytes=52 * 2**20
        ),
    )(
        fresh_keys.reshape(batch, block, size),
        fresh_values.reshape(batch, block, size),
        turn_angle.T,
        key_gain.reshape(1, size),
    )
    return (
        out_keys.reshape(1, 1, size, length),
        out_values.reshape(1, length, 1, size),
        out_scale.reshape(1, 1, size),
    )


def solution(mesh):
    in_specs = (
        P(None, ("coarse", "fine"), "group", None),
        P(None, ("coarse", "fine"), "group", None),
        P(),
        P(),
    )
    out_specs = (
        P(("coarse", "fine"), "group", None, None),
        P(("coarse", "fine"), None, "group", None),
        P(("coarse", "fine"), "group", None),
    )
    return jax.shard_map(local, mesh=mesh, in_specs=in_specs, out_specs=out_specs, check_vma=False)
```

```python
import jax
import jax.numpy as jnp
from jax import lax
from jax.experimental import pallas as pl
from jax.experimental.pallas import tpu as pltpu
from jax.sharding import PartitionSpec as P

MESH = pl.DeviceIdType.MESH
COARSE, FINE = 4, 8
PARTS = COARSE * FINE
CHUNK = 128
PIECES = 1
EARLY = 1
KEYS, VALUES = 0, 1
LAG = 3
AHEAD = 4
OFFSETS = (4, 3, -3, 2, -2, 1, -1, 0)
FORWARD4 = ((0, 2), (1, 3))


def coarse_plan():
    plan = []
    for array in (KEYS, VALUES):
        plan += [[(array, 1, o), (array, 3, o)] for o in OFFSETS]
        plan += [[(array, 2, o)] for o in OFFSETS]
    return plan


def fine_plan(way):
    ready = {e: j + LAG + (e[1] == 2) for j, step in enumerate(coarse_plan()) for e in step}
    waiting = []
    for array in (KEYS, VALUES):
        for rows in range(COARSE):
            for hops in range(1, FINE // 2 + 1):
                if hops == FINE // 2 and (rows in FORWARD4[array]) != (way == 1):
                    continue
                off = hops if hops == FINE // 2 else way * hops
                waiting.append((ready.get((array, rows, off), 0), array, hops, rows, 0))
    plan = []
    while waiting:
        now = len(plan)
        best = min(
            (w for w in waiting if w[0] <= now), key=lambda w: (w[1], w[4] - w[2], w[0], w[3])
        )
        waiting.remove(best)
        plan.append(best[1:])
        _, array, hops, rows, done = best
        if done + 1 < hops:
            waiting.append((now + LAG, array, hops, rows, done + 1))
    return plan


COARSE_PLAN = coarse_plan()
FINE_PLAN = {way: fine_plan(way) for way in (1, -1)}
STEPS = len(FINE_PLAN[1])
TWO_AWAY = next(j for j, step in enumerate(COARSE_PLAN) if step[0][1] == 2)
SLOT = {}
for _step in COARSE_PLAN:
    for _array, _rows, _off in _step:
        if _off:
            SLOT["staged", _array, _rows, _off] = len(SLOT)
for _way in FINE_PLAN:
    for _array, _hops, _rows, _done in FINE_PLAN[_way]:
        if _done:
            SLOT["passing", _way, _array, _hops, _rows, _done] = len(SLOT)
for _way in FINE_PLAN:
    for _array, _hops, _rows, _done in FINE_PLAN[_way][:EARLY]:
        SLOT["early", _way, _array, _hops] = len(SLOT)
SLOTS = len(SLOT)
FIRST_TURN = STEPS // 2 + LAG + 1
TURNS = 2
FIRST_NARROW = FIRST_TURN + PARTS // TURNS
NARROWS = 4


def kernel(keys, values, angle, gain, out_keys, out_values, out_scale,
           held, turned, angles, peak, gains, gain_row, box,
           sent, box_came, key_came, value_came, local_sem, beyond):
    c, f, g = (lax.axis_index(name) for name in ("coarse", "fine", "group"))
    block = held.shape[1]
    me = c * FINE + f
    source_of = (keys, values)
    final_of = (held, out_values)

    def at(row, column):
        return ((c + row) % COARSE, (f + column + FINE) % FINE, g)

    near = [(0, 1), (0, -1), (1, 0), (3, 0)]
    barrier = pltpu.get_barrier_semaphore()
    for row, column in near:
        pl.semaphore_signal(barrier, inc=1, device_id=at(row, column), device_id_type=MESH)
    for way in FINE_PLAN:
        for array, hops, _, _ in FINE_PLAN[way][:EARLY]:
            slot = SLOT["early", way, array, hops]
            off = hops if hops == FINE // 2 else way * hops
            pltpu.make_async_copy(
                source_of[array].at[c * FINE + (f + off + FINE) % FINE], box.at[slot], box_came.at[slot]
            ).start()
    pl.semaphore_wait(barrier, len(near))
    pl.semaphore_signal(beyond, inc=1, device_id=at(1, 0), device_id_type=MESH)

    def came(array, device):
        return key_came.at[device] if array == KEYS else value_came

    def send_coarse(array, rows, off):
        there = at(rows, 0)
        if off:
            slot = SLOT["staged", array, rows, off]
            target, arrived = box.at[slot], box_came.at[slot]
        else:
            target, arrived = final_of[array].at[me], came(array, me)
        pltpu.make_async_remote_copy(
            src_ref=source_of[array].at[there[0] * FINE + (f + off + FINE) % FINE],
            dst_ref=target, send_sem=sent, recv_sem=arrived, device_id=there, device_id_type=MESH,
        ).start()

    def send_fine(way, array, hops, rows, done):
        off = hops if hops == FINE // 2 else way * hops
        if done:
            slot = SLOT["passing", way, array, hops, rows, done]
        elif rows:
            slot = SLOT["staged", array, rows, off]
        else:
            slot = SLOT.get(("early", way, array, hops))
        if slot is None:
            source = source_of[array].at[c * FINE + (f + off + FINE) % FINE]
        else:
            source = box.at[slot]
            pltpu.make_async_copy(source, source, box_came.at[slot]).wait()
        if done + 1 < hops:
            slot = SLOT["passing", way, array, hops, rows, done + 1]
            target, arrived = box.at[slot], box_came.at[slot]
        else:
            home = ((c + COARSE - rows) % COARSE) * FINE + (f - way * done + FINE) % FINE
            target, arrived = final_of[array].at[home], came(array, home)
        pltpu.make_async_remote_copy(
            src_ref=source, dst_ref=target, send_sem=sent, recv_sem=arrived,
            device_id=at(0, way), device_id_type=MESH,
        ).start()

    def exchange(step):
        for way in FINE_PLAN:
            send_fine(way, *FINE_PLAN[way][step])
        if step == 0:
            for entry in sum(COARSE_PLAN[:AHEAD], []):
                send_coarse(*entry)
        if step + AHEAD == TWO_AWAY:
            pl.semaphore_wait(beyond, 1)
        if step + AHEAD < len(COARSE_PLAN):
            for entry in COARSE_PLAN[step + AHEAD]:
                send_coarse(*entry)

    def turn(source):
        @pl.loop(0, block // CHUNK)
        def _(n):
            plain = held[source, pl.ds(pl.multiple_of(n * CHUNK, CHUNK), CHUNK), :]
            wide = plain.astype(jnp.float32).T
            mean = jnp.sum(wide * wide, axis=0, keepdims=True) * (1.0 / wide.shape[0])
            wide = wide * lax.rsqrt(mean + 1e-06) * gains[...]
            where = pl.ds(pl.multiple_of(source * block + n * CHUNK, CHUNK), CHUNK)
            a = angles[:, where]
            cosine, sine = jnp.cos(a), jnp.sin(a)
            half = a.shape[0]
            first, second = wide[:half], wide[half:]
            low = first * cosine - second * sine
            high = second * cosine + first * sine
            turned[:half, where] = low
            turned[half:, where] = high
            peak[:half] = jnp.maximum(peak[:half], jnp.abs(low))
            peak[half:] = jnp.maximum(peak[half:], jnp.abs(high))

    def narrow(i):
        where = pl.ds(pl.multiple_of(i * block, block), block)
        scale = jnp.max(peak[...], axis=1, keepdims=True)
        out_keys[:, where] = (turned[:, where] / scale).astype(out_keys.dtype)

    own_keys = pltpu.make_async_copy(keys.at[me], held.at[me], local_sem.at[0])
    own_values = pltpu.make_async_copy(values.at[me], out_values.at[me], local_sem.at[1])
    get_gain = pltpu.make_async_copy(gain, gain_row, local_sem.at[3])
    get_angles = pltpu.make_async_copy(angle, angles, local_sem.at[2])
    for step in range(FIRST_TURN):
        exchange(step)
        if step == 2:
            own_keys.start()
            own_values.start()
            get_angles.start()
            get_gain.start()
    peak[...] = jnp.zeros_like(peak)
    get_gain.wait()
    gains[...] = jnp.broadcast_to(gain_row[...], gains.shape).T
    own_keys.wait()
    own_values.wait()
    get_angles.wait()
    for i in range(1, PARTS):
        source = (me + i) % PARTS
        pltpu.make_async_copy(held.at[source], held.at[source], key_came.at[source]).wait()

    @pl.loop(FIRST_TURN, STEPS)
    def _(step):
        for k in range(FIRST_TURN, STEPS):
            @pl.when(step == k)
            def _():
                exchange(k)

        @pl.when(step < FIRST_NARROW)
        def _():
            @pl.loop(0, TURNS)
            def _(i):
                turn((step - FIRST_TURN) * TURNS + i)

        @pl.when((step >= FIRST_NARROW) & (step < FIRST_NARROW + PARTS // NARROWS))
        def _():
            @pl.loop(0, NARROWS)
            def _(i):
                narrow((step - FIRST_NARROW) * NARROWS + i)

    out_scale[...] = jnp.max(peak[...].T, axis=0, keepdims=True)
    whole = pl.ds(0, PARTS)
    sends = sum(len(s) for s in COARSE_PLAN) + 2 * STEPS
    for _ in range(sends // PARTS):
        pltpu.make_async_copy(values.at[whole], values.at[whole], sent).wait()
    if sends % PARTS:
        rest = pl.ds(0, sends % PARTS)
        pltpu.make_async_copy(values.at[rest], values.at[rest], sent).wait()
    rest = pl.ds(0, PARTS - 1)
    pltpu.make_async_copy(values.at[rest], values.at[rest], value_came).wait()


def store(keys, values, scale, out_keys, out_values, out_scale, done):
    copies = [pltpu.make_async_copy(scale, out_scale, done.at[0])]
    for a, (held, out) in enumerate(((keys, out_keys), (values, out_values))):
        rows = held.shape[0] // PIECES
        for i in range(PIECES):
            piece = pl.ds(i * rows, rows)
            copies.append(
                pltpu.make_async_copy(held.at[piece], out.at[piece], done.at[1 + a * PIECES + i])
            )
    for copy in copies:
        copy.start()
    for copy in copies:
        copy.wait()


def local(fresh_keys, fresh_values, turn_angle, key_gain):
    batch, block, _, size = fresh_keys.shape
    length = turn_angle.shape[0]
    hbm = pl.BlockSpec(memory_space=pltpu.HBM)
    vmem = pl.BlockSpec(memory_space=pltpu.VMEM)
    out_keys, out_values, out_scale = pl.pallas_call(
        kernel,
        name="exchange",
        out_shape=[
            pltpu.VMEM((size, length), jnp.bfloat16),
            pltpu.VMEM((batch, block, size), jnp.bfloat16),
            pltpu.VMEM((1, size), jnp.float32),
        ],
        in_specs=[hbm, hbm, hbm, hbm],
        out_specs=[vmem, vmem, vmem],
        scratch_shapes=[
            pltpu.VMEM((batch, block, size), jnp.bfloat16),
            pltpu.VMEM((size, length), jnp.float32),
            pltpu.VMEM((size // 2, length), jnp.float32),
            pltpu.VMEM((size, CHUNK), jnp.float32),
            pltpu.VMEM((size, CHUNK), jnp.float32),
            pltpu.VMEM((1, size), jnp.float32),
            pltpu.VMEM((SLOTS, block, size), jnp.bfloat16),
            pltpu.SemaphoreType.DMA,
            pltpu.SemaphoreType.DMA((SLOTS,)),
            pltpu.SemaphoreType.DMA((PARTS,)),
            pltpu.SemaphoreType.DMA,
            pltpu.SemaphoreType.DMA((4,)),
            pltpu.SemaphoreType.REGULAR,
        ],
        compiler_params=pltpu.CompilerParams(
            collective_id=0, has_side_effects=True, vmem_limit_bytes=52 * 2**20
        ),
    )(
        fresh_keys.reshape(batch, block, size),
        fresh_values.reshape(batch, block, size),
        turn_angle.T,
        key_gain.reshape(1, size),
    )
    out_keys, out_values, out_scale = pl.pallas_call(
        store,
        name="store",
        out_shape=[
            jax.ShapeDtypeStruct((size, length), jnp.bfloat16),
            jax.ShapeDtypeStruct((batch, block, size), jnp.bfloat16),
            jax.ShapeDtypeStruct((1, size), jnp.float32),
        ],
        in_specs=[vmem, vmem, vmem],
        out_specs=[hbm, hbm, hbm],
        scratch_shapes=[pltpu.SemaphoreType.DMA((1 + 2 * PIECES,))],
        compiler_params=pltpu.CompilerParams(vmem_limit_bytes=16 * 2**20),
    )(out_keys, out_values, out_scale)
    return (
        out_keys.reshape(1, 1, size, length),
        out_values.reshape(1, length, 1, size),
        out_scale.reshape(1, 1, size),
    )


def solution(mesh):
    in_specs = (
        P(None, ("coarse", "fine"), "group", None),
        P(None, ("coarse", "fine"), "group", None),
        P(),
        P(),
    )
    out_specs = (
        P(("coarse", "fine"), "group", None, None),
        P(("coarse", "fine"), None, "group", None),
        P(("coarse", "fine"), "group", None),
    )
    return jax.shard_map(local, mesh=mesh, in_specs=in_specs, out_specs=out_specs, check_vma=False)
```

```python
import jax
import jax.numpy as jnp
from jax import lax
from jax.experimental import pallas as pl
from jax.experimental.pallas import tpu as pltpu
from jax.sharding import PartitionSpec as P

MESH = pl.DeviceIdType.MESH
COARSE, FINE = 4, 8
PARTS = COARSE * FINE
CHUNK = 128
PIECES = 1
EARLY = 1
KEYS, VALUES = 0, 1
LAG = 3
AHEAD = 4
OFFSETS = (4, 3, -3, 2, -2, 1, -1, 0)
FORWARD4 = ((0, 2), (1, 3))


def coarse_plan():
    plan = []
    for array in (KEYS, VALUES):
        plan += [[(array, 1, o), (array, 3, o)] for o in OFFSETS]
        plan += [[(array, 2, o)] for o in OFFSETS]
    return plan


def fine_plan(way):
    ready = {e: j + LAG + (e[1] == 2) for j, step in enumerate(coarse_plan()) for e in step}
    waiting = []
    for array in (KEYS, VALUES):
        for rows in range(COARSE):
            for hops in range(1, FINE // 2 + 1):
                if hops == FINE // 2 and (rows in FORWARD4[array]) != (way == 1):
                    continue
                off = hops if hops == FINE // 2 else way * hops
                waiting.append((ready.get((array, rows, off), 0), array, hops, rows, 0))
    plan = []
    while waiting:
        now = len(plan)
        best = min(
            (w for w in waiting if w[0] <= now), key=lambda w: (w[1], w[4] - w[2], w[0], w[3])
        )
        waiting.remove(best)
        plan.append(best[1:])
        _, array, hops, rows, done = best
        if done + 1 < hops:
            waiting.append((now + LAG, array, hops, rows, done + 1))
    return plan


COARSE_PLAN = coarse_plan()
FINE_PLAN = {way: fine_plan(way) for way in (1, -1)}
STEPS = len(FINE_PLAN[1])
SLOT = {}
for _step in COARSE_PLAN:
    for _array, _rows, _off in _step:
        if _off:
            SLOT["staged", _array, _rows, _off] = len(SLOT)
for _way in FINE_PLAN:
    for _array, _hops, _rows, _done in FINE_PLAN[_way]:
        if _done:
            SLOT["passing", _way, _array, _hops, _rows, _done] = len(SLOT)
for _way in FINE_PLAN:
    for _array, _hops, _rows, _done in FINE_PLAN[_way][:EARLY]:
        SLOT["early", _way, _array, _hops] = len(SLOT)
SLOTS = len(SLOT)
FIRST_TURN = STEPS // 2 + LAG + 1
TURNS = 2
FIRST_NARROW = FIRST_TURN + PARTS // TURNS
NARROWS = 4


def kernel(keys, values, angle, gain, out_keys, out_values, out_scale,
           held, turned, angles, peak, gains, gain_row, box,
           sent, box_came, key_came, value_came, local_sem, beyond):
    c, f, g = (lax.axis_index(name) for name in ("coarse", "fine", "group"))
    block = held.shape[1]
    me = c * FINE + f
    source_of = (keys, values)
    final_of = (held, out_values)

    def at(row, column):
        return ((c + row) % COARSE, (f + column + FINE) % FINE, g)

    barrier = pltpu.get_barrier_semaphore()
    last = COARSE - 1

    def greet(semaphore, rows, column=0):
        pl.semaphore_signal(
            semaphore, inc=1, device_id=at(rows, column), device_id_type=MESH
        )

    greet(barrier, 0, 1)
    greet(barrier, 0, -1)
    pl.when(c > 0)(lambda: greet(barrier, last))
    pl.when(c < last)(lambda: greet(barrier, 1))
    for way in FINE_PLAN:
        for array, hops, _, _ in FINE_PLAN[way][:EARLY]:
            slot = SLOT["early", way, array, hops]
            off = hops if hops == FINE // 2 else way * hops
            pltpu.make_async_copy(
                source_of[array].at[c * FINE + (f + off + FINE) % FINE], box.at[slot], box_came.at[slot]
            ).start()
    pl.semaphore_wait(barrier, 2 + (c + last) // COARSE + (2 * last - c) // COARSE)
    inner = (c > 0) & (c < last)

    @pl.when(inner)
    def _():
        greet(beyond, last)
        greet(beyond, 1)

    def greet_the_rest():
        @pl.when(inner)
        def _():
            pl.semaphore_wait(beyond, 1)

        pl.when(c == 1)(lambda: greet(beyond, last))
        pl.when(c == last - 1)(lambda: greet(beyond, 1))
        pl.when((c == 0) | (c == last))(lambda: pl.semaphore_wait(beyond, 2))

    def came(array, device):
        return key_came.at[device] if array == KEYS else value_came

    def send_coarse(array, rows, off):
        there = at(rows, 0)
        if off:
            slot = SLOT["staged", array, rows, off]
            target, arrived = box.at[slot], box_came.at[slot]
        else:
            target, arrived = final_of[array].at[me], came(array, me)
        pltpu.make_async_remote_copy(
            src_ref=source_of[array].at[there[0] * FINE + (f + off + FINE) % FINE],
            dst_ref=target, send_sem=sent, recv_sem=arrived, device_id=there, device_id_type=MESH,
        ).start()

    def send_fine(way, array, hops, rows, done):
        off = hops if hops == FINE // 2 else way * hops
        if done:
            slot = SLOT["passing", way, array, hops, rows, done]
        elif rows:
            slot = SLOT["staged", array, rows, off]
        else:
            slot = SLOT.get(("early", way, array, hops))
        if slot is None:
            source = source_of[array].at[c * FINE + (f + off + FINE) % FINE]
        else:
            source = box.at[slot]
            pltpu.make_async_copy(source, source, box_came.at[slot]).wait()
        if done + 1 < hops:
            slot = SLOT["passing", way, array, hops, rows, done + 1]
            target, arrived = box.at[slot], box_came.at[slot]
        else:
            home = ((c + COARSE - rows) % COARSE) * FINE + (f - way * done + FINE) % FINE
            target, arrived = final_of[array].at[home], came(array, home)
        pltpu.make_async_remote_copy(
            src_ref=source, dst_ref=target, send_sem=sent, recv_sem=arrived,
            device_id=at(0, way), device_id_type=MESH,
        ).start()

    def exchange(step):
        for way in FINE_PLAN:
            send_fine(way, *FINE_PLAN[way][step])
        if step < LAG - 1:
            return
        if step == LAG - 1:
            greet_the_rest()
            for entry in sum(COARSE_PLAN[: AHEAD + step], []):
                send_coarse(*entry)
        if step + AHEAD < len(COARSE_PLAN):
            for entry in COARSE_PLAN[step + AHEAD]:
                send_coarse(*entry)

    def turn(source):
        @pl.loop(0, block // CHUNK)
        def _(n):
            plain = held[source, pl.ds(pl.multiple_of(n * CHUNK, CHUNK), CHUNK), :]
            wide = plain.astype(jnp.float32).T
            mean = jnp.sum(wide * wide, axis=0, keepdims=True) * (1.0 / wide.shape[0])
            wide = wide * lax.rsqrt(mean + 1e-06) * gains[...]
            where = pl.ds(pl.multiple_of(source * block + n * CHUNK, CHUNK), CHUNK)
            a = angles[:, where]
            cosine, sine = jnp.cos(a), jnp.sin(a)
            half = a.shape[0]
            first, second = wide[:half], wide[half:]
            low = first * cosine - second * sine
            high = second * cosine + first * sine
            turned[:half, where] = low
            turned[half:, where] = high
            peak[:half] = jnp.maximum(peak[:half], jnp.abs(low))
            peak[half:] = jnp.maximum(peak[half:], jnp.abs(high))

    def narrow(i):
        where = pl.ds(pl.multiple_of(i * block, block), block)
        scale = jnp.max(peak[...], axis=1, keepdims=True)
        out_keys[:, where] = (turned[:, where] / scale).astype(out_keys.dtype)

    own_keys = pltpu.make_async_copy(keys.at[me], held.at[me], local_sem.at[0])
    own_values = pltpu.make_async_copy(values.at[me], out_values.at[me], local_sem.at[1])
    get_gain = pltpu.make_async_copy(gain, gain_row, local_sem.at[3])
    get_angles = pltpu.make_async_copy(angle, angles, local_sem.at[2])
    for step in range(FIRST_TURN):
        exchange(step)
        if step == 2:
            own_keys.start()
            own_values.start()
            get_angles.start()
            get_gain.start()
    peak[...] = jnp.zeros_like(peak)
    get_gain.wait()
    gains[...] = jnp.broadcast_to(gain_row[...], gains.shape).T
    own_keys.wait()
    own_values.wait()
    get_angles.wait()
    for i in range(1, PARTS):
        source = (me + i) % PARTS
        pltpu.make_async_copy(held.at[source], held.at[source], key_came.at[source]).wait()

    @pl.loop(FIRST_TURN, STEPS)
    def _(step):
        for k in range(FIRST_TURN, STEPS):
            @pl.when(step == k)
            def _():
                exchange(k)

        @pl.when(step < FIRST_NARROW)
        def _():
            @pl.loop(0, TURNS)
            def _(i):
                turn((step - FIRST_TURN) * TURNS + i)

        @pl.when((step >= FIRST_NARROW) & (step < FIRST_NARROW + PARTS // NARROWS))
        def _():
            @pl.loop(0, NARROWS)
            def _(i):
                narrow((step - FIRST_NARROW) * NARROWS + i)

    out_scale[...] = jnp.max(peak[...].T, axis=0, keepdims=True)
    whole = pl.ds(0, PARTS)
    sends = sum(len(s) for s in COARSE_PLAN) + 2 * STEPS
    for _ in range(sends // PARTS):
        pltpu.make_async_copy(values.at[whole], values.at[whole], sent).wait()
    if sends % PARTS:
        rest = pl.ds(0, sends % PARTS)
        pltpu.make_async_copy(values.at[rest], values.at[rest], sent).wait()
    rest = pl.ds(0, PARTS - 1)
    pltpu.make_async_copy(values.at[rest], values.at[rest], value_came).wait()


def store(keys, values, scale, out_keys, out_values, out_scale, done):
    copies = [pltpu.make_async_copy(scale, out_scale, done.at[0])]
    for a, (held, out) in enumerate(((keys, out_keys), (values, out_values))):
        rows = held.shape[0] // PIECES
        for i in range(PIECES):
            piece = pl.ds(i * rows, rows)
            copies.append(
                pltpu.make_async_copy(held.at[piece], out.at[piece], done.at[1 + a * PIECES + i])
            )
    for copy in copies:
        copy.start()
    for copy in copies:
        copy.wait()


def local(fresh_keys, fresh_values, turn_angle, key_gain):
    batch, block, _, size = fresh_keys.shape
    length = turn_angle.shape[0]
    hbm = pl.BlockSpec(memory_space=pltpu.HBM)
    vmem = pl.BlockSpec(memory_space=pltpu.VMEM)
    out_keys, out_values, out_scale = pl.pallas_call(
        kernel,
        name="exchange",
        out_shape=[
            pltpu.VMEM((size, length), jnp.bfloat16),
            pltpu.VMEM((batch, block, size), jnp.bfloat16),
            pltpu.VMEM((1, size), jnp.float32),
        ],
        in_specs=[hbm, hbm, hbm, hbm],
        out_specs=[vmem, vmem, vmem],
        scratch_shapes=[
            pltpu.VMEM((batch, block, size), jnp.bfloat16),
            pltpu.VMEM((size, length), jnp.float32),
            pltpu.VMEM((size // 2, length), jnp.float32),
            pltpu.VMEM((size, CHUNK), jnp.float32),
            pltpu.VMEM((size, CHUNK), jnp.float32),
            pltpu.VMEM((1, size), jnp.float32),
            pltpu.VMEM((SLOTS, block, size), jnp.bfloat16),
            pltpu.SemaphoreType.DMA,
            pltpu.SemaphoreType.DMA((SLOTS,)),
            pltpu.SemaphoreType.DMA((PARTS,)),
            pltpu.SemaphoreType.DMA,
            pltpu.SemaphoreType.DMA((4,)),
            pltpu.SemaphoreType.REGULAR,
        ],
        compiler_params=pltpu.CompilerParams(
            collective_id=0, has_side_effects=True, vmem_limit_bytes=52 * 2**20
        ),
    )(
        fresh_keys.reshape(batch, block, size),
        fresh_values.reshape(batch, block, size),
        turn_angle.T,
        key_gain.reshape(1, size),
    )
    out_keys, out_values, out_scale = pl.pallas_call(
        store,
        name="store",
        out_shape=[
            jax.ShapeDtypeStruct((size, length), jnp.bfloat16),
            jax.ShapeDtypeStruct((batch, block, size), jnp.bfloat16),
            jax.ShapeDtypeStruct((1, size), jnp.float32),
        ],
        in_specs=[vmem, vmem, vmem],
        out_specs=[hbm, hbm, hbm],
        scratch_shapes=[pltpu.SemaphoreType.DMA((1 + 2 * PIECES,))],
        compiler_params=pltpu.CompilerParams(vmem_limit_bytes=16 * 2**20),
    )(out_keys, out_values, out_scale)
    return (
        out_keys.reshape(1, 1, size, length),
        out_values.reshape(1, length, 1, size),
        out_scale.reshape(1, 1, size),
    )


def solution(mesh):
    in_specs = (
        P(None, ("coarse", "fine"), "group", None),
        P(None, ("coarse", "fine"), "group", None),
        P(),
        P(),
    )
    out_specs = (
        P(("coarse", "fine"), "group", None, None),
        P(("coarse", "fine"), None, "group", None),
        P(("coarse", "fine"), "group", None),
    )
    return jax.shard_map(local, mesh=mesh, in_specs=in_specs, out_specs=out_specs, check_vma=False)
```

```python
import jax
import jax.numpy as jnp
from jax import lax
from jax.experimental import pallas as pl
from jax.experimental.pallas import tpu as pltpu
from jax.sharding import PartitionSpec as P

MESH = pl.DeviceIdType.MESH
COARSE, FINE = 4, 8
PARTS = COARSE * FINE
CHUNK = 128
PIECES = 1
EARLY = 1
KEYS, VALUES = 0, 1
LAG = 3
AHEAD = 4
OFFSETS = (4, 3, -3, 2, -2, 1, -1, 0)
FORWARD4 = ((0, 2), (1, 3))


def coarse_plan():
    plan = []
    for array in (KEYS, VALUES):
        plan += [[(array, 1, o), (array, 3, o)] for o in OFFSETS]
        plan += [[(array, 2, o)] for o in OFFSETS]
    return plan


def fine_plan(way):
    ready = {e: j + LAG + (e[1] == 2) for j, step in enumerate(coarse_plan()) for e in step}
    waiting = []
    for array in (KEYS, VALUES):
        for rows in range(COARSE):
            for hops in range(1, FINE // 2 + 1):
                if hops == FINE // 2 and (rows in FORWARD4[array]) != (way == 1):
                    continue
                off = hops if hops == FINE // 2 else way * hops
                waiting.append((ready.get((array, rows, off), 0), array, hops, rows, 0))
    plan = []
    while waiting:
        now = len(plan)
        best = min(
            (w for w in waiting if w[0] <= now), key=lambda w: (w[1], w[4] - w[2], w[0], w[3])
        )
        waiting.remove(best)
        plan.append(best[1:])
        _, array, hops, rows, done = best
        if done + 1 < hops:
            waiting.append((now + LAG, array, hops, rows, done + 1))
    return plan


COARSE_PLAN = coarse_plan()
FINE_PLAN = {way: fine_plan(way) for way in (1, -1)}
STEPS = len(FINE_PLAN[1])
SLOT = {}
for _step in COARSE_PLAN:
    for _array, _rows, _off in _step:
        if _off:
            SLOT["staged", _array, _rows, _off] = len(SLOT)
for _way in FINE_PLAN:
    for _array, _hops, _rows, _done in FINE_PLAN[_way]:
        if _done:
            SLOT["passing", _way, _array, _hops, _rows, _done] = len(SLOT)
for _way in FINE_PLAN:
    for _array, _hops, _rows, _done in FINE_PLAN[_way][:EARLY]:
        SLOT["early", _way, _array, _hops] = len(SLOT)
SPLIT = {1: (FORWARD4[VALUES][0], 4), -1: (0, 3)}
for _way in SPLIT:
    for _own in (True, False):
        for _done in range(1, FINE // 2):
            SLOT["half", _way, _own, _done] = len(SLOT)
SLOTS = len(SLOT)
HALF_SENDS = {
    key: n
    for n, key in enumerate(
        (way, part, done) for way in SPLIT for part in range(3) for done in range(FINE // 2)
    )
}
FIRST_TURN = STEPS // 2 + LAG + 1
TURNS = 2
FIRST_NARROW = FIRST_TURN + PARTS // TURNS
NARROWS = 4


def kernel(keys, values, angle, gain, out_keys, out_values, out_scale,
           held, turned, angles, peak, gains, gain_row, box,
           sent, half_sent, box_came, key_came, value_came, local_sem, beyond):
    c, f, g = (lax.axis_index(name) for name in ("coarse", "fine", "group"))
    block = held.shape[1]
    me = c * FINE + f
    source_of = (keys, values)
    final_of = (held, out_values)

    def at(row, column):
        return ((c + row) % COARSE, (f + column + FINE) % FINE, g)

    barrier = pltpu.get_barrier_semaphore()
    last = COARSE - 1

    def greet(semaphore, rows, column=0):
        pl.semaphore_signal(
            semaphore, inc=1, device_id=at(rows, column), device_id_type=MESH
        )

    greet(barrier, 0, 1)
    greet(barrier, 0, -1)
    pl.when(c > 0)(lambda: greet(barrier, last))
    pl.when(c < last)(lambda: greet(barrier, 1))
    for way in FINE_PLAN:
        for array, hops, _, _ in FINE_PLAN[way][:EARLY]:
            slot = SLOT["early", way, array, hops]
            off = hops if hops == FINE // 2 else way * hops
            pltpu.make_async_copy(
                source_of[array].at[c * FINE + (f + off + FINE) % FINE], box.at[slot], box_came.at[slot]
            ).start()
    pl.semaphore_wait(barrier, 2 + (c + last) // COARSE + (2 * last - c) // COARSE)
    inner = (c > 0) & (c < last)

    @pl.when(inner)
    def _():
        greet(beyond, last)
        greet(beyond, 1)

    def greet_the_rest():
        @pl.when(inner)
        def _():
            pl.semaphore_wait(beyond, 1)

        pl.when(c == 1)(lambda: greet(beyond, last))
        pl.when(c == last - 1)(lambda: greet(beyond, 1))
        pl.when((c == 0) | (c == last))(lambda: pl.semaphore_wait(beyond, 2))

    def came(array, device):
        return key_came.at[device] if array == KEYS else value_came

    def send_coarse(array, rows, off):
        there = at(rows, 0)
        if off:
            slot = SLOT["staged", array, rows, off]
            target, arrived = box.at[slot], box_came.at[slot]
        else:
            target, arrived = final_of[array].at[me], came(array, me)
        pltpu.make_async_remote_copy(
            src_ref=source_of[array].at[there[0] * FINE + (f + off + FINE) % FINE],
            dst_ref=target, send_sem=sent, recv_sem=arrived, device_id=there, device_id_type=MESH,
        ).start()

    def send_fine(way, array, hops, rows, done):
        off = hops if hops == FINE // 2 else way * hops
        if done:
            slot = SLOT["passing", way, array, hops, rows, done]
        elif rows:
            slot = SLOT["staged", array, rows, off]
        else:
            slot = SLOT.get(("early", way, array, hops))
        if slot is None:
            source = source_of[array].at[c * FINE + (f + off + FINE) % FINE]
        else:
            source = box.at[slot]
            pltpu.make_async_copy(source, source, box_came.at[slot]).wait()
        if done + 1 < hops:
            slot = SLOT["passing", way, array, hops, rows, done + 1]
            target, arrived = box.at[slot], box_came.at[slot]
        else:
            home = ((c + COARSE - rows) % COARSE) * FINE + (f - way * done + FINE) % FINE
            target, arrived = final_of[array].at[home], came(array, home)
        pltpu.make_async_remote_copy(
            src_ref=source, dst_ref=target, send_sem=sent, recv_sem=arrived,
            device_id=at(0, way), device_id_type=MESH,
        ).start()

    def half_send(way, part, done, act):
        home_column = (f - way * done + FINE) % FINE
        if part == 0:
            act()
        elif part == 1:
            pl.when(home_column != SPLIT[way][1])(act)
        else:
            pl.when(home_column == SPLIT[-way][1])(act)

    def send_split(way, done):
        for part in range(3):
            rows = SPLIT[way if part < 2 else -way][0]
            piece = pl.ds(0 if part == 0 else block // 2, block // 2)

            def act(part=part, rows=rows, piece=piece):
                hops, array = FINE // 2, VALUES

                def passing(at_hop):
                    if part == 0:
                        return SLOT["passing", way, array, hops, rows, at_hop]
                    return SLOT["half", way, part == 1, at_hop]

                if done:
                    slot = passing(done)
                    source = box.at[slot, piece]
                    pltpu.make_async_copy(source, source, box_came.at[slot]).wait()
                elif rows:
                    slot = SLOT["staged", array, rows, hops]
                    if part == 0:
                        whole = box.at[slot]
                        pltpu.make_async_copy(whole, whole, box_came.at[slot]).wait()
                    source = box.at[slot, piece]
                else:
                    source = source_of[array].at[c * FINE + (f + hops) % FINE, piece]
                if done + 1 < hops:
                    slot = passing(done + 1)
                    target, arrived = box.at[slot, piece], box_came.at[slot]
                else:
                    home = ((c + COARSE - rows) % COARSE) * FINE + (f - way * done + FINE) % FINE
                    target, arrived = final_of[array].at[home, piece], value_came
                pltpu.make_async_remote_copy(
                    src_ref=source, dst_ref=target, send_sem=half_sent.at[HALF_SENDS[way, part, done]],
                    recv_sem=arrived, device_id=at(0, way), device_id_type=MESH,
                ).start()

            half_send(way, part, done, act)

    def exchange(step):
        for way in FINE_PLAN:
            array, hops, rows, done = FINE_PLAN[way][step]
            if (array, hops, rows) == (VALUES, FINE // 2, SPLIT[way][0]):
                send_split(way, done)
            else:
                send_fine(way, array, hops, rows, done)
        if step < LAG - 1:
            return
        if step == LAG - 1:
            greet_the_rest()
            for entry in sum(COARSE_PLAN[: AHEAD + step], []):
                send_coarse(*entry)
        if step + AHEAD < len(COARSE_PLAN):
            for entry in COARSE_PLAN[step + AHEAD]:
                send_coarse(*entry)

    def turn(source):
        @pl.loop(0, block // CHUNK)
        def _(n):
            plain = held[source, pl.ds(pl.multiple_of(n * CHUNK, CHUNK), CHUNK), :]
            wide = plain.astype(jnp.float32).T
            mean = jnp.sum(wide * wide, axis=0, keepdims=True) * (1.0 / wide.shape[0])
            wide = wide * lax.rsqrt(mean + 1e-06) * gains[...]
            where = pl.ds(pl.multiple_of(source * block + n * CHUNK, CHUNK), CHUNK)
            a = angles[:, where]
            cosine, sine = jnp.cos(a), jnp.sin(a)
            half = a.shape[0]
            first, second = wide[:half], wide[half:]
            low = first * cosine - second * sine
            high = second * cosine + first * sine
            turned[:half, where] = low
            turned[half:, where] = high
            peak[:half] = jnp.maximum(peak[:half], jnp.abs(low))
            peak[half:] = jnp.maximum(peak[half:], jnp.abs(high))

    def narrow(i):
        where = pl.ds(pl.multiple_of(i * block, block), block)
        scale = jnp.max(peak[...], axis=1, keepdims=True)
        out_keys[:, where] = (turned[:, where] / scale).astype(out_keys.dtype)

    own_keys = pltpu.make_async_copy(keys.at[me], held.at[me], local_sem.at[0])
    own_values = pltpu.make_async_copy(values.at[me], out_values.at[me], local_sem.at[1])
    get_gain = pltpu.make_async_copy(gain, gain_row, local_sem.at[3])
    get_angles = pltpu.make_async_copy(angle, angles, local_sem.at[2])
    for step in range(FIRST_TURN):
        exchange(step)
        if step == 2:
            own_keys.start()
            own_values.start()
            get_angles.start()
            get_gain.start()
    peak[...] = jnp.zeros_like(peak)
    get_gain.wait()
    gains[...] = jnp.broadcast_to(gain_row[...], gains.shape).T
    own_keys.wait()
    own_values.wait()
    get_angles.wait()
    for i in range(1, PARTS):
        source = (me + i) % PARTS
        pltpu.make_async_copy(held.at[source], held.at[source], key_came.at[source]).wait()

    @pl.loop(FIRST_TURN, STEPS)
    def _(step):
        for k in range(FIRST_TURN, STEPS):
            @pl.when(step == k)
            def _():
                exchange(k)

        @pl.when(step < FIRST_NARROW)
        def _():
            @pl.loop(0, TURNS)
            def _(i):
                turn((step - FIRST_TURN) * TURNS + i)

        @pl.when((step >= FIRST_NARROW) & (step < FIRST_NARROW + PARTS // NARROWS))
        def _():
            @pl.loop(0, NARROWS)
            def _(i):
                narrow((step - FIRST_NARROW) * NARROWS + i)

    out_scale[...] = jnp.max(peak[...].T, axis=0, keepdims=True)
    whole = pl.ds(0, PARTS)
    sends = sum(len(s) for s in COARSE_PLAN) + 2 * STEPS - 2 * (FINE // 2)
    for _ in range(sends // PARTS):
        pltpu.make_async_copy(values.at[whole], values.at[whole], sent).wait()
    if sends % PARTS:
        rest = pl.ds(0, sends % PARTS)
        pltpu.make_async_copy(values.at[rest], values.at[rest], sent).wait()
    for (way, part, done), n in HALF_SENDS.items():
        half = values.at[0, pl.ds(0, block // 2)]
        half_send(
            way, part, done, lambda n=n: pltpu.make_async_copy(half, half, half_sent.at[n]).wait()
        )
    rest = pl.ds(0, PARTS - 1)
    pltpu.make_async_copy(values.at[rest], values.at[rest], value_came).wait()


def store(keys, values, scale, out_keys, out_values, out_scale, done):
    copies = [pltpu.make_async_copy(scale, out_scale, done.at[0])]
    for a, (held, out) in enumerate(((keys, out_keys), (values, out_values))):
        rows = held.shape[0] // PIECES
        for i in range(PIECES):
            piece = pl.ds(i * rows, rows)
            copies.append(
                pltpu.make_async_copy(held.at[piece], out.at[piece], done.at[1 + a * PIECES + i])
            )
    for copy in copies:
        copy.start()
    for copy in copies:
        copy.wait()


def local(fresh_keys, fresh_values, turn_angle, key_gain):
    batch, block, _, size = fresh_keys.shape
    length = turn_angle.shape[0]
    hbm = pl.BlockSpec(memory_space=pltpu.HBM)
    vmem = pl.BlockSpec(memory_space=pltpu.VMEM)
    out_keys, out_values, out_scale = pl.pallas_call(
        kernel,
        name="exchange",
        out_shape=[
            pltpu.VMEM((size, length), jnp.bfloat16),
            pltpu.VMEM((batch, block, size), jnp.bfloat16),
            pltpu.VMEM((1, size), jnp.float32),
        ],
        in_specs=[hbm, hbm, hbm, hbm],
        out_specs=[vmem, vmem, vmem],
        scratch_shapes=[
            pltpu.VMEM((batch, block, size), jnp.bfloat16),
            pltpu.VMEM((size, length), jnp.float32),
            pltpu.VMEM((size // 2, length), jnp.float32),
            pltpu.VMEM((size, CHUNK), jnp.float32),
            pltpu.VMEM((size, CHUNK), jnp.float32),
            pltpu.VMEM((1, size), jnp.float32),
            pltpu.VMEM((SLOTS, block, size), jnp.bfloat16),
            pltpu.SemaphoreType.DMA,
            pltpu.SemaphoreType.DMA((len(HALF_SENDS),)),
            pltpu.SemaphoreType.DMA((SLOTS,)),
            pltpu.SemaphoreType.DMA((PARTS,)),
            pltpu.SemaphoreType.DMA,
            pltpu.SemaphoreType.DMA((4,)),
            pltpu.SemaphoreType.REGULAR,
        ],
        compiler_params=pltpu.CompilerParams(
            collective_id=0, has_side_effects=True, vmem_limit_bytes=52 * 2**20
        ),
    )(
        fresh_keys.reshape(batch, block, size),
        fresh_values.reshape(batch, block, size),
        turn_angle.T,
        key_gain.reshape(1, size),
    )
    out_keys, out_values, out_scale = pl.pallas_call(
        store,
        name="store",
        out_shape=[
            jax.ShapeDtypeStruct((size, length), jnp.bfloat16),
            jax.ShapeDtypeStruct((batch, block, size), jnp.bfloat16),
            jax.ShapeDtypeStruct((1, size), jnp.float32),
        ],
        in_specs=[vmem, vmem, vmem],
        out_specs=[hbm, hbm, hbm],
        scratch_shapes=[pltpu.SemaphoreType.DMA((1 + 2 * PIECES,))],
        compiler_params=pltpu.CompilerParams(vmem_limit_bytes=16 * 2**20),
    )(out_keys, out_values, out_scale)
    return (
        out_keys.reshape(1, 1, size, length),
        out_values.reshape(1, length, 1, size),
        out_scale.reshape(1, 1, size),
    )


def solution(mesh):
    in_specs = (
        P(None, ("coarse", "fine"), "group", None),
        P(None, ("coarse", "fine"), "group", None),
        P(),
        P(),
    )
    out_specs = (
        P(("coarse", "fine"), "group", None, None),
        P(("coarse", "fine"), None, "group", None),
        P(("coarse", "fine"), "group", None),
    )
    return jax.shard_map(local, mesh=mesh, in_specs=in_specs, out_specs=out_specs, check_vma=False)
```

```python
import jax
import jax.numpy as jnp
from jax import lax
from jax.experimental import pallas as pl
from jax.experimental.pallas import tpu as pltpu
from jax.sharding import PartitionSpec as P

MESH = pl.DeviceIdType.MESH
COARSE, FINE = 4, 8
PARTS = COARSE * FINE
CHUNK = 128
PIECES = 1
EARLY = 1
KEYS, VALUES = 0, 1
LAG = 3
AHEAD = 4
OFFSETS = (4, 3, -3, 2, -2, 1, -1, 0)
FORWARD4 = ((0, 2), (1, 3))


def coarse_plan():
    plan = []
    for array in (KEYS, VALUES):
        plan += [[(array, 1, o), (array, 3, o)] for o in OFFSETS]
        plan += [[(array, 2, o)] for o in OFFSETS]
    return plan


def fine_plan(way):
    ready = {e: j + LAG + (e[1] == 2) for j, step in enumerate(coarse_plan()) for e in step}
    waiting = []
    for array in (KEYS, VALUES):
        for rows in range(COARSE):
            for hops in range(1, FINE // 2 + 1):
                if hops == FINE // 2 and (rows in FORWARD4[array]) != (way == 1):
                    continue
                off = hops if hops == FINE // 2 else way * hops
                waiting.append((ready.get((array, rows, off), 0), array, hops, rows, 0))
    plan = []
    while waiting:
        now = len(plan)
        best = min(
            (w for w in waiting if w[0] <= now), key=lambda w: (w[1], w[4] - w[2], w[0], w[3])
        )
        waiting.remove(best)
        plan.append(best[1:])
        _, array, hops, rows, done = best
        if done + 1 < hops:
            waiting.append((now + LAG, array, hops, rows, done + 1))
    return plan


COARSE_PLAN = coarse_plan()
FINE_PLAN = {way: fine_plan(way) for way in (1, -1)}
STEPS = len(FINE_PLAN[1])
SLOT = {}
for _step in COARSE_PLAN:
    for _array, _rows, _off in _step:
        if _off:
            SLOT["staged", _array, _rows, _off] = len(SLOT)
for _way in FINE_PLAN:
    for _array, _hops, _rows, _done in FINE_PLAN[_way]:
        if _done:
            SLOT["passing", _way, _array, _hops, _rows, _done] = len(SLOT)
for _way in FINE_PLAN:
    for _array, _hops, _rows, _done in FINE_PLAN[_way][:EARLY]:
        SLOT["early", _way, _array, _hops] = len(SLOT)
SPLIT = {1: (FORWARD4[VALUES][0], 4), -1: (0, 3)}
for _way in SPLIT:
    for _own in (True, False):
        for _done in range(1, FINE // 2):
            SLOT["half", _way, _own, _done] = len(SLOT)
SLOTS = len(SLOT)
HALF_SENDS = {
    key: n
    for n, key in enumerate(
        (way, part, done) for way in SPLIT for part in range(3) for done in range(FINE // 2)
    )
}
FIRST_TURN = STEPS // 2 + LAG + 1
TURNS = 2
FIRST_NARROW = FIRST_TURN + PARTS // TURNS
NARROWS = 4


def kernel(keys, values, angle, gain, out_keys, out_values, out_scale,
           held, turned, angles, peak, gains, gain_row, box,
           sent, half_sent, box_came, key_came, value_came, local_sem, beyond, ready):
    c, f, g = (lax.axis_index(name) for name in ("coarse", "fine", "group"))
    block = held.shape[1]
    me = c * FINE + f
    source_of = (keys, values)
    final_of = (held, out_values)

    def at(row, column):
        return ((c + row) % COARSE, (f + column + FINE) % FINE, g)

    barrier = pltpu.get_barrier_semaphore()
    last, end = COARSE - 1, FINE - 1

    def greet(semaphore, rows, column=0):
        pl.semaphore_signal(
            semaphore, inc=1, device_id=at(rows, column), device_id_type=MESH
        )

    pl.when(f < end - 1)(lambda: greet(barrier, 0, 1))
    pl.when((f == 0) | (f == end))(lambda: greet(barrier, 0, -1))
    pl.when(c < last)(lambda: greet(barrier, 1))
    for way in FINE_PLAN:
        for array, hops, _, _ in FINE_PLAN[way][:EARLY]:
            slot = SLOT["early", way, array, hops]
            off = hops if hops == FINE // 2 else way * hops
            pltpu.make_async_copy(
                source_of[array].at[c * FINE + (f + off + FINE) % FINE], box.at[slot], box_came.at[slot]
            ).start()
    heard = (f + end) // FINE + f // (end - 1) - f // end + (c + last) // COARSE
    pl.when((f > 0) | (c > 0))(lambda: pl.semaphore_wait(barrier, heard))
    pl.when((f > 0) & (f < end))(lambda: greet(ready.at[0], 0, -1))
    pl.when(f >= end - 1)(lambda: greet(ready.at[1], 0, 1))
    pl.when(c > 0)(lambda: greet(ready.at[2], last))
    inner = (c > 0) & (c < last)

    def greet_the_rest():
        pl.when(c < last)(lambda: pl.semaphore_wait(ready.at[2], 1))

        @pl.when(inner)
        def _():
            greet(beyond, last)
            greet(beyond, 1)
            pl.semaphore_wait(beyond, 1)

        pl.when(c == 1)(lambda: greet(beyond, last))
        pl.when(c == last - 1)(lambda: greet(beyond, 1))
        pl.when((c == 0) | (c == last))(lambda: pl.semaphore_wait(beyond, 2))

    def came(array, device):
        return key_came.at[device] if array == KEYS else value_came

    def send_coarse(array, rows, off):
        there = at(rows, 0)
        if off:
            slot = SLOT["staged", array, rows, off]
            target, arrived = box.at[slot], box_came.at[slot]
        else:
            target, arrived = final_of[array].at[me], came(array, me)
        pltpu.make_async_remote_copy(
            src_ref=source_of[array].at[there[0] * FINE + (f + off + FINE) % FINE],
            dst_ref=target, send_sem=sent, recv_sem=arrived, device_id=there, device_id_type=MESH,
        ).start()

    def send_fine(way, array, hops, rows, done):
        off = hops if hops == FINE // 2 else way * hops
        if done:
            slot = SLOT["passing", way, array, hops, rows, done]
        elif rows:
            slot = SLOT["staged", array, rows, off]
        else:
            slot = SLOT.get(("early", way, array, hops))
        if slot is None:
            source = source_of[array].at[c * FINE + (f + off + FINE) % FINE]
        else:
            source = box.at[slot]
            pltpu.make_async_copy(source, source, box_came.at[slot]).wait()
        if done + 1 < hops:
            slot = SLOT["passing", way, array, hops, rows, done + 1]
            target, arrived = box.at[slot], box_came.at[slot]
        else:
            home = ((c + COARSE - rows) % COARSE) * FINE + (f - way * done + FINE) % FINE
            target, arrived = final_of[array].at[home], came(array, home)
        pltpu.make_async_remote_copy(
            src_ref=source, dst_ref=target, send_sem=sent, recv_sem=arrived,
            device_id=at(0, way), device_id_type=MESH,
        ).start()

    def half_send(way, part, done, act):
        home_column = (f - way * done + FINE) % FINE
        if part == 0:
            act()
        elif part == 1:
            pl.when(home_column != SPLIT[way][1])(act)
        else:
            pl.when(home_column == SPLIT[-way][1])(act)

    def send_split(way, done):
        for part in range(3):
            rows = SPLIT[way if part < 2 else -way][0]
            piece = pl.ds(0 if part == 0 else block // 2, block // 2)

            def act(part=part, rows=rows, piece=piece):
                hops, array = FINE // 2, VALUES

                def passing(at_hop):
                    if part == 0:
                        return SLOT["passing", way, array, hops, rows, at_hop]
                    return SLOT["half", way, part == 1, at_hop]

                if done:
                    slot = passing(done)
                    source = box.at[slot, piece]
                    pltpu.make_async_copy(source, source, box_came.at[slot]).wait()
                elif rows:
                    slot = SLOT["staged", array, rows, hops]
                    if part == 0:
                        whole = box.at[slot]
                        pltpu.make_async_copy(whole, whole, box_came.at[slot]).wait()
                    source = box.at[slot, piece]
                else:
                    source = source_of[array].at[c * FINE + (f + hops) % FINE, piece]
                if done + 1 < hops:
                    slot = passing(done + 1)
                    target, arrived = box.at[slot, piece], box_came.at[slot]
                else:
                    home = ((c + COARSE - rows) % COARSE) * FINE + (f - way * done + FINE) % FINE
                    target, arrived = final_of[array].at[home, piece], value_came
                pltpu.make_async_remote_copy(
                    src_ref=source, dst_ref=target, send_sem=half_sent.at[HALF_SENDS[way, part, done]],
                    recv_sem=arrived, device_id=at(0, way), device_id_type=MESH,
                ).start()

            half_send(way, part, done, act)

    def exchange(step):
        for way in FINE_PLAN:
            array, hops, rows, done = FINE_PLAN[way][step]
            if (array, hops, rows) == (VALUES, FINE // 2, SPLIT[way][0]):
                send_split(way, done)
            else:
                send_fine(way, array, hops, rows, done)
        if step + AHEAD < len(COARSE_PLAN):
            for entry in COARSE_PLAN[step + AHEAD]:
                send_coarse(*entry)

    def turn(source):
        @pl.loop(0, block // CHUNK)
        def _(n):
            plain = held[source, pl.ds(pl.multiple_of(n * CHUNK, CHUNK), CHUNK), :]
            wide = plain.astype(jnp.float32).T
            mean = jnp.sum(wide * wide, axis=0, keepdims=True) * (1.0 / wide.shape[0])
            wide = wide * lax.rsqrt(mean + 1e-06) * gains[...]
            where = pl.ds(pl.multiple_of(source * block + n * CHUNK, CHUNK), CHUNK)
            a = angles[:, where]
            cosine, sine = jnp.cos(a), jnp.sin(a)
            half = a.shape[0]
            first, second = wide[:half], wide[half:]
            low = first * cosine - second * sine
            high = second * cosine + first * sine
            turned[:half, where] = low
            turned[half:, where] = high
            peak[:half] = jnp.maximum(peak[:half], jnp.abs(low))
            peak[half:] = jnp.maximum(peak[half:], jnp.abs(high))

    def narrow(i):
        where = pl.ds(pl.multiple_of(i * block, block), block)
        scale = jnp.max(peak[...], axis=1, keepdims=True)
        out_keys[:, where] = (turned[:, where] / scale).astype(out_keys.dtype)

    def first_sends(way):
        for step in range(LAG):
            send_fine(way, *FINE_PLAN[way][step])

    pl.when((f > 0) & (f < end))(lambda: first_sends(-1))
    pl.when(f < end - 1)(lambda: pl.semaphore_wait(ready.at[0], 1))
    first_sends(1)

    @pl.when((f == 0) | (f == end))
    def _():
        pl.semaphore_wait(ready.at[1], 1)
        first_sends(-1)

    greet_the_rest()
    for entry in sum(COARSE_PLAN[: AHEAD + LAG], []):
        send_coarse(*entry)
    own_keys = pltpu.make_async_copy(keys.at[me], held.at[me], local_sem.at[0])
    own_values = pltpu.make_async_copy(values.at[me], out_values.at[me], local_sem.at[1])
    get_gain = pltpu.make_async_copy(gain, gain_row, local_sem.at[3])
    get_angles = pltpu.make_async_copy(angle, angles, local_sem.at[2])
    own_keys.start()
    own_values.start()
    get_angles.start()
    get_gain.start()
    for step in range(LAG, FIRST_TURN):
        exchange(step)
    peak[...] = jnp.zeros_like(peak)
    get_gain.wait()
    gains[...] = jnp.broadcast_to(gain_row[...], gains.shape).T
    own_keys.wait()
    own_values.wait()
    get_angles.wait()
    for i in range(1, PARTS):
        source = (me + i) % PARTS
        pltpu.make_async_copy(held.at[source], held.at[source], key_came.at[source]).wait()

    @pl.loop(FIRST_TURN, STEPS)
    def _(step):
        for k in range(FIRST_TURN, STEPS):
            @pl.when(step == k)
            def _():
                exchange(k)

        @pl.when(step < FIRST_NARROW)
        def _():
            @pl.loop(0, TURNS)
            def _(i):
                turn((step - FIRST_TURN) * TURNS + i)

        @pl.when((step >= FIRST_NARROW) & (step < FIRST_NARROW + PARTS // NARROWS))
        def _():
            @pl.loop(0, NARROWS)
            def _(i):
                narrow((step - FIRST_NARROW) * NARROWS + i)

    out_scale[...] = jnp.max(peak[...].T, axis=0, keepdims=True)
    whole = pl.ds(0, PARTS)
    sends = sum(len(s) for s in COARSE_PLAN) + 2 * STEPS - 2 * (FINE // 2)
    for _ in range(sends // PARTS):
        pltpu.make_async_copy(values.at[whole], values.at[whole], sent).wait()
    if sends % PARTS:
        rest = pl.ds(0, sends % PARTS)
        pltpu.make_async_copy(values.at[rest], values.at[rest], sent).wait()
    for (way, part, done), n in HALF_SENDS.items():
        half = values.at[0, pl.ds(0, block // 2)]
        half_send(
            way, part, done, lambda n=n: pltpu.make_async_copy(half, half, half_sent.at[n]).wait()
        )
    rest = pl.ds(0, PARTS - 1)
    pltpu.make_async_copy(values.at[rest], values.at[rest], value_came).wait()


def store(keys, values, scale, out_keys, out_values, out_scale, done):
    copies = [pltpu.make_async_copy(scale, out_scale, done.at[0])]
    for a, (held, out) in enumerate(((keys, out_keys), (values, out_values))):
        rows = held.shape[0] // PIECES
        for i in range(PIECES):
            piece = pl.ds(i * rows, rows)
            copies.append(
                pltpu.make_async_copy(held.at[piece], out.at[piece], done.at[1 + a * PIECES + i])
            )
    for copy in copies:
        copy.start()
    for copy in copies:
        copy.wait()


def local(fresh_keys, fresh_values, turn_angle, key_gain):
    batch, block, _, size = fresh_keys.shape
    length = turn_angle.shape[0]
    hbm = pl.BlockSpec(memory_space=pltpu.HBM)
    vmem = pl.BlockSpec(memory_space=pltpu.VMEM)
    out_keys, out_values, out_scale = pl.pallas_call(
        kernel,
        name="exchange",
        out_shape=[
            pltpu.VMEM((size, length), jnp.bfloat16),
            pltpu.VMEM((batch, block, size), jnp.bfloat16),
            pltpu.VMEM((1, size), jnp.float32),
        ],
        in_specs=[hbm, hbm, hbm, hbm],
        out_specs=[vmem, vmem, vmem],
        scratch_shapes=[
            pltpu.VMEM((batch, block, size), jnp.bfloat16),
            pltpu.VMEM((size, length), jnp.float32),
            pltpu.VMEM((size // 2, length), jnp.float32),
            pltpu.VMEM((size, CHUNK), jnp.float32),
            pltpu.VMEM((size, CHUNK), jnp.float32),
            pltpu.VMEM((1, size), jnp.float32),
            pltpu.VMEM((SLOTS, block, size), jnp.bfloat16),
            pltpu.SemaphoreType.DMA,
            pltpu.SemaphoreType.DMA((len(HALF_SENDS),)),
            pltpu.SemaphoreType.DMA((SLOTS,)),
            pltpu.SemaphoreType.DMA((PARTS,)),
            pltpu.SemaphoreType.DMA,
            pltpu.SemaphoreType.DMA((4,)),
            pltpu.SemaphoreType.REGULAR,
            pltpu.SemaphoreType.REGULAR((3,)),
        ],
        compiler_params=pltpu.CompilerParams(
            collective_id=0, has_side_effects=True, vmem_limit_bytes=52 * 2**20
        ),
    )(
        fresh_keys.reshape(batch, block, size),
        fresh_values.reshape(batch, block, size),
        turn_angle.T,
        key_gain.reshape(1, size),
    )
    out_keys, out_values, out_scale = pl.pallas_call(
        store,
        name="store",
        out_shape=[
            jax.ShapeDtypeStruct((size, length), jnp.bfloat16),
            jax.ShapeDtypeStruct((batch, block, size), jnp.bfloat16),
            jax.ShapeDtypeStruct((1, size), jnp.float32),
        ],
        in_specs=[vmem, vmem, vmem],
        out_specs=[hbm, hbm, hbm],
        scratch_shapes=[pltpu.SemaphoreType.DMA((1 + 2 * PIECES,))],
        compiler_params=pltpu.CompilerParams(vmem_limit_bytes=16 * 2**20),
    )(out_keys, out_values, out_scale)
    return (
        out_keys.reshape(1, 1, size, length),
        out_values.reshape(1, length, 1, size),
        out_scale.reshape(1, 1, size),
    )


def solution(mesh):
    in_specs = (
        P(None, ("coarse", "fine"), "group", None),
        P(None, ("coarse", "fine"), "group", None),
        P(),
        P(),
    )
    out_specs = (
        P(("coarse", "fine"), "group", None, None),
        P(("coarse", "fine"), None, "group", None),
        P(("coarse", "fine"), "group", None),
    )
    return jax.shard_map(local, mesh=mesh, in_specs=in_specs, out_specs=out_specs, check_vma=False)
```

```python
import jax
import jax.numpy as jnp
from jax import lax
from jax.experimental import pallas as pl
from jax.experimental.pallas import tpu as pltpu
from jax.sharding import PartitionSpec as P

MESH = pl.DeviceIdType.MESH
COARSE, FINE = 4, 8
PARTS = COARSE * FINE
CHUNK = 128
PIECES = 2
EARLY = 1
KEYS, VALUES = 0, 1
LAG = 3
AHEAD = 4
OFFSETS = (4, 3, -3, 2, -2, 1, -1, 0)
FORWARD4 = ((0, 2), (1, 3))


def coarse_plan():
    plan = []
    for array in (KEYS, VALUES):
        plan += [[(array, 1, o), (array, 3, o)] for o in OFFSETS]
        plan += [[(array, 2, o)] for o in OFFSETS]
    return plan


def fine_plan(way):
    ready = {e: j + LAG + (e[1] == 2) for j, step in enumerate(coarse_plan()) for e in step}
    waiting = []
    for array in (KEYS, VALUES):
        for rows in range(COARSE):
            for hops in range(1, FINE // 2 + 1):
                if hops == FINE // 2 and (rows in FORWARD4[array]) != (way == 1):
                    continue
                off = hops if hops == FINE // 2 else way * hops
                waiting.append((ready.get((array, rows, off), 0), array, hops, rows, 0))
    plan = []
    while waiting:
        now = len(plan)
        best = min(
            (w for w in waiting if w[0] <= now), key=lambda w: (w[1], w[4] - w[2], w[0], w[3])
        )
        waiting.remove(best)
        plan.append(best[1:])
        _, array, hops, rows, done = best
        if done + 1 < hops:
            waiting.append((now + LAG, array, hops, rows, done + 1))
    return plan


COARSE_PLAN = coarse_plan()
FINE_PLAN = {way: fine_plan(way) for way in (1, -1)}
STEPS = len(FINE_PLAN[1])
SLOT = {}
for _step in COARSE_PLAN:
    for _array, _rows, _off in _step:
        if _off:
            SLOT["staged", _array, _rows, _off] = len(SLOT)
for _way in FINE_PLAN:
    for _array, _hops, _rows, _done in FINE_PLAN[_way]:
        if _done:
            SLOT["passing", _way, _array, _hops, _rows, _done] = len(SLOT)
for _way in FINE_PLAN:
    for _array, _hops, _rows, _done in FINE_PLAN[_way][:EARLY]:
        SLOT["early", _way, _array, _hops] = len(SLOT)
SPLIT = {1: (FORWARD4[VALUES][0], 4), -1: (0, 3)}
for _way in SPLIT:
    for _own in (True, False):
        for _done in range(1, FINE // 2):
            SLOT["half", _way, _own, _done] = len(SLOT)
SLOTS = len(SLOT)
HALF_SENDS = {
    key: n
    for n, key in enumerate(
        (way, part, done) for way in SPLIT for part in range(3) for done in range(FINE // 2)
    )
}
FIRST_TURN = STEPS // 2 + LAG + 1
TURNS = 2
FIRST_NARROW = FIRST_TURN + PARTS // TURNS
NARROWS = 4


def kernel(keys, values, angle, gain, out_keys, out_values, out_scale,
           held, turned, angles, peak, gains, gain_row, box,
           sent, half_sent, box_came, key_came, value_came, local_sem, beyond, ready):
    c, f, g = (lax.axis_index(name) for name in ("coarse", "fine", "group"))
    block = held.shape[1]
    me = c * FINE + f
    source_of = (keys, values)
    final_of = (held, out_values)

    def at(row, column):
        return ((c + row) % COARSE, (f + column + FINE) % FINE, g)

    barrier = pltpu.get_barrier_semaphore()
    last, end = COARSE - 1, FINE - 1

    def greet(semaphore, rows, column=0):
        pl.semaphore_signal(
            semaphore, inc=1, device_id=at(rows, column), device_id_type=MESH
        )

    pl.when(f < end - 1)(lambda: greet(barrier, 0, 1))
    pl.when((f == 0) | (f == end))(lambda: greet(barrier, 0, -1))
    pl.when(c < last)(lambda: greet(barrier, 1))
    for way in FINE_PLAN:
        for array, hops, _, _ in FINE_PLAN[way][:EARLY]:
            slot = SLOT["early", way, array, hops]
            off = hops if hops == FINE // 2 else way * hops
            pltpu.make_async_copy(
                source_of[array].at[c * FINE + (f + off + FINE) % FINE], box.at[slot], box_came.at[slot]
            ).start()
    heard = (f + end) // FINE + f // (end - 1) - f // end + (c + last) // COARSE
    pl.when((f > 0) | (c > 0))(lambda: pl.semaphore_wait(barrier, heard))
    pl.when((f > 0) & (f < end))(lambda: greet(ready.at[0], 0, -1))
    pl.when(f >= end - 1)(lambda: greet(ready.at[1], 0, 1))
    pl.when(c > 0)(lambda: greet(ready.at[2], last))
    inner = (c > 0) & (c < last)

    def greet_the_rest():
        pl.when(c < last)(lambda: pl.semaphore_wait(ready.at[2], 1))

        @pl.when(inner)
        def _():
            greet(beyond, last)
            greet(beyond, 1)
            pl.semaphore_wait(beyond, 1)

        pl.when(c == 1)(lambda: greet(beyond, last))
        pl.when(c == last - 1)(lambda: greet(beyond, 1))
        pl.when((c == 0) | (c == last))(lambda: pl.semaphore_wait(beyond, 2))

    def came(array, device):
        return key_came.at[device] if array == KEYS else value_came

    def send_coarse(array, rows, off):
        there = at(rows, 0)
        if off:
            slot = SLOT["staged", array, rows, off]
            target, arrived = box.at[slot], box_came.at[slot]
        else:
            target, arrived = final_of[array].at[me], came(array, me)
        pltpu.make_async_remote_copy(
            src_ref=source_of[array].at[there[0] * FINE + (f + off + FINE) % FINE],
            dst_ref=target, send_sem=sent, recv_sem=arrived, device_id=there, device_id_type=MESH,
        ).start()

    def send_fine(way, array, hops, rows, done):
        off = hops if hops == FINE // 2 else way * hops
        if done:
            slot = SLOT["passing", way, array, hops, rows, done]
        elif rows:
            slot = SLOT["staged", array, rows, off]
        else:
            slot = SLOT.get(("early", way, array, hops))
        if slot is None:
            source = source_of[array].at[c * FINE + (f + off + FINE) % FINE]
        else:
            source = box.at[slot]
            pltpu.make_async_copy(source, source, box_came.at[slot]).wait()
        if done + 1 < hops:
            slot = SLOT["passing", way, array, hops, rows, done + 1]
            target, arrived = box.at[slot], box_came.at[slot]
        else:
            home = ((c + COARSE - rows) % COARSE) * FINE + (f - way * done + FINE) % FINE
            target, arrived = final_of[array].at[home], came(array, home)
        pltpu.make_async_remote_copy(
            src_ref=source, dst_ref=target, send_sem=sent, recv_sem=arrived,
            device_id=at(0, way), device_id_type=MESH,
        ).start()

    def half_send(way, part, done, act):
        home_column = (f - way * done + FINE) % FINE
        if part == 0:
            act()
        elif part == 1:
            pl.when(home_column != SPLIT[way][1])(act)
        else:
            pl.when(home_column == SPLIT[-way][1])(act)

    def send_split(way, done):
        for part in range(3):
            rows = SPLIT[way if part < 2 else -way][0]
            piece = pl.ds(0 if part == 0 else block // 2, block // 2)

            def act(part=part, rows=rows, piece=piece):
                hops, array = FINE // 2, VALUES

                def passing(at_hop):
                    if part == 0:
                        return SLOT["passing", way, array, hops, rows, at_hop]
                    return SLOT["half", way, part == 1, at_hop]

                if done:
                    slot = passing(done)
                    source = box.at[slot, piece]
                    pltpu.make_async_copy(source, source, box_came.at[slot]).wait()
                elif rows:
                    slot = SLOT["staged", array, rows, hops]
                    if part == 0:
                        whole = box.at[slot]
                        pltpu.make_async_copy(whole, whole, box_came.at[slot]).wait()
                    source = box.at[slot, piece]
                else:
                    source = source_of[array].at[c * FINE + (f + hops) % FINE, piece]
                if done + 1 < hops:
                    slot = passing(done + 1)
                    target, arrived = box.at[slot, piece], box_came.at[slot]
                else:
                    home = ((c + COARSE - rows) % COARSE) * FINE + (f - way * done + FINE) % FINE
                    target, arrived = final_of[array].at[home, piece], value_came
                pltpu.make_async_remote_copy(
                    src_ref=source, dst_ref=target, send_sem=half_sent.at[HALF_SENDS[way, part, done]],
                    recv_sem=arrived, device_id=at(0, way), device_id_type=MESH,
                ).start()

            half_send(way, part, done, act)

    def exchange(step):
        for way in FINE_PLAN:
            array, hops, rows, done = FINE_PLAN[way][step]
            if (array, hops, rows) == (VALUES, FINE // 2, SPLIT[way][0]):
                send_split(way, done)
            else:
                send_fine(way, array, hops, rows, done)
        if step + AHEAD < len(COARSE_PLAN):
            for entry in COARSE_PLAN[step + AHEAD]:
                send_coarse(*entry)

    def turn(source):
        @pl.loop(0, block // CHUNK)
        def _(n):
            plain = held[source, pl.ds(pl.multiple_of(n * CHUNK, CHUNK), CHUNK), :]
            wide = plain.astype(jnp.float32).T
            mean = jnp.sum(wide * wide, axis=0, keepdims=True) * (1.0 / wide.shape[0])
            wide = wide * lax.rsqrt(mean + 1e-06) * gains[...]
            where = pl.ds(pl.multiple_of(source * block + n * CHUNK, CHUNK), CHUNK)
            a = angles[:, where]
            cosine, sine = jnp.cos(a), jnp.sin(a)
            half = a.shape[0]
            first, second = wide[:half], wide[half:]
            low = first * cosine - second * sine
            high = second * cosine + first * sine
            turned[:half, where] = low
            turned[half:, where] = high
            peak[:half] = jnp.maximum(peak[:half], jnp.abs(low))
            peak[half:] = jnp.maximum(peak[half:], jnp.abs(high))

    def narrow(i):
        where = pl.ds(pl.multiple_of(i * block, block), block)
        scale = jnp.max(peak[...], axis=1, keepdims=True)
        out_keys[:, where] = (turned[:, where] / scale).astype(out_keys.dtype)

    def first_sends(way):
        for step in range(LAG):
            send_fine(way, *FINE_PLAN[way][step])

    pl.when((f > 0) & (f < end))(lambda: first_sends(-1))
    pl.when(f < end - 1)(lambda: pl.semaphore_wait(ready.at[0], 1))
    first_sends(1)

    @pl.when((f == 0) | (f == end))
    def _():
        pl.semaphore_wait(ready.at[1], 1)
        first_sends(-1)

    greet_the_rest()
    for entry in sum(COARSE_PLAN[: AHEAD + LAG], []):
        send_coarse(*entry)
    own_keys = pltpu.make_async_copy(keys.at[me], held.at[me], local_sem.at[0])
    own_values = pltpu.make_async_copy(values.at[me], out_values.at[me], local_sem.at[1])
    get_gain = pltpu.make_async_copy(gain, gain_row, local_sem.at[3])
    get_angles = pltpu.make_async_copy(angle, angles, local_sem.at[2])
    own_keys.start()
    own_values.start()
    get_angles.start()
    get_gain.start()
    for step in range(LAG, FIRST_TURN):
        exchange(step)
    peak[...] = jnp.zeros_like(peak)
    get_gain.wait()
    gains[...] = jnp.broadcast_to(gain_row[...], gains.shape).T
    own_keys.wait()
    own_values.wait()
    get_angles.wait()
    for i in range(1, PARTS):
        source = (me + i) % PARTS
        pltpu.make_async_copy(held.at[source], held.at[source], key_came.at[source]).wait()

    @pl.loop(FIRST_TURN, STEPS)
    def _(step):
        for k in range(FIRST_TURN, STEPS):
            @pl.when(step == k)
            def _():
                exchange(k)

        @pl.when(step < FIRST_NARROW)
        def _():
            @pl.loop(0, TURNS)
            def _(i):
                turn((step - FIRST_TURN) * TURNS + i)

        @pl.when((step >= FIRST_NARROW) & (step < FIRST_NARROW + PARTS // NARROWS))
        def _():
            @pl.loop(0, NARROWS)
            def _(i):
                narrow((step - FIRST_NARROW) * NARROWS + i)

    out_scale[...] = jnp.max(peak[...].T, axis=0, keepdims=True)
    whole = pl.ds(0, PARTS)
    sends = sum(len(s) for s in COARSE_PLAN) + 2 * STEPS - 2 * (FINE // 2)
    for _ in range(sends // PARTS):
        pltpu.make_async_copy(values.at[whole], values.at[whole], sent).wait()
    if sends % PARTS:
        rest = pl.ds(0, sends % PARTS)
        pltpu.make_async_copy(values.at[rest], values.at[rest], sent).wait()
    for (way, part, done), n in HALF_SENDS.items():
        half = values.at[0, pl.ds(0, block // 2)]
        half_send(
            way, part, done, lambda n=n: pltpu.make_async_copy(half, half, half_sent.at[n]).wait()
        )
    rest = pl.ds(0, PARTS - 1)
    pltpu.make_async_copy(values.at[rest], values.at[rest], value_came).wait()


def store(keys, values, scale, out_keys, out_values, out_scale, done):
    copies = [pltpu.make_async_copy(scale, out_scale, done.at[0])]
    for a, (held, out) in enumerate(((keys, out_keys), (values, out_values))):
        rows = held.shape[0] // PIECES
        for i in range(PIECES):
            piece = pl.ds(i * rows, rows)
            copies.append(
                pltpu.make_async_copy(held.at[piece], out.at[piece], done.at[1 + a * PIECES + i])
            )
    for i, copy in enumerate(copies):
        copy.start(priority=i % 2)
    for copy in copies:
        copy.wait()


def local(fresh_keys, fresh_values, turn_angle, key_gain):
    batch, block, _, size = fresh_keys.shape
    length = turn_angle.shape[0]
    hbm = pl.BlockSpec(memory_space=pltpu.HBM)
    vmem = pl.BlockSpec(memory_space=pltpu.VMEM)
    out_keys, out_values, out_scale = pl.pallas_call(
        kernel,
        name="exchange",
        out_shape=[
            pltpu.VMEM((size, length), jnp.bfloat16),
            pltpu.VMEM((batch, block, size), jnp.bfloat16),
            pltpu.VMEM((1, size), jnp.float32),
        ],
        in_specs=[hbm, hbm, hbm, hbm],
        out_specs=[vmem, vmem, vmem],
        scratch_shapes=[
            pltpu.VMEM((batch, block, size), jnp.bfloat16),
            pltpu.VMEM((size, length), jnp.float32),
            pltpu.VMEM((size // 2, length), jnp.float32),
            pltpu.VMEM((size, CHUNK), jnp.float32),
            pltpu.VMEM((size, CHUNK), jnp.float32),
            pltpu.VMEM((1, size), jnp.float32),
            pltpu.VMEM((SLOTS, block, size), jnp.bfloat16),
            pltpu.SemaphoreType.DMA,
            pltpu.SemaphoreType.DMA((len(HALF_SENDS),)),
            pltpu.SemaphoreType.DMA((SLOTS,)),
            pltpu.SemaphoreType.DMA((PARTS,)),
            pltpu.SemaphoreType.DMA,
            pltpu.SemaphoreType.DMA((4,)),
            pltpu.SemaphoreType.REGULAR,
            pltpu.SemaphoreType.REGULAR((3,)),
        ],
        compiler_params=pltpu.CompilerParams(
            collective_id=0, has_side_effects=True, vmem_limit_bytes=52 * 2**20
        ),
    )(
        fresh_keys.reshape(batch, block, size),
        fresh_values.reshape(batch, block, size),
        turn_angle.T,
        key_gain.reshape(1, size),
    )
    out_keys, out_values, out_scale = pl.pallas_call(
        store,
        name="store",
        out_shape=[
            jax.ShapeDtypeStruct((size, length), jnp.bfloat16),
            jax.ShapeDtypeStruct((batch, block, size), jnp.bfloat16),
            jax.ShapeDtypeStruct((1, size), jnp.float32),
        ],
        in_specs=[vmem, vmem, vmem],
        out_specs=[hbm, hbm, hbm],
        scratch_shapes=[pltpu.SemaphoreType.DMA((1 + 2 * PIECES,))],
        compiler_params=pltpu.CompilerParams(vmem_limit_bytes=16 * 2**20),
    )(out_keys, out_values, out_scale)
    return (
        out_keys.reshape(1, 1, size, length),
        out_values.reshape(1, length, 1, size),
        out_scale.reshape(1, 1, size),
    )


def solution(mesh):
    in_specs = (
        P(None, ("coarse", "fine"), "group", None),
        P(None, ("coarse", "fine"), "group", None),
        P(),
        P(),
    )
    out_specs = (
        P(("coarse", "fine"), "group", None, None),
        P(("coarse", "fine"), None, "group", None),
        P(("coarse", "fine"), "group", None),
    )
    return jax.shard_map(local, mesh=mesh, in_specs=in_specs, out_specs=out_specs, check_vma=False)
```
